32 devices in a mesh: dp: 16 (over z, y, x), tensor: 2 (over core).
Axes of the slice: x: 2, y: 2, z: 4, core: 2. Of those that a mesh axis runs over, the one named last changes fastest.
Arguments:
- image_tokens: bfloat16 [32, 577, 1024], P('dp'), may hold values from -6 to 6
- first_gain: float32 [1024], replicated, may hold values from 0.5 to 1.5
- first_shift: float32 [1024], replicated, may hold values from -1.5 to 1.5
- w_qkv: bfloat16 [1024, 3, 1024], P(None, None, 'tensor'), may hold values from -8 to 8, as said below
- query_value_bias: float32 [2, 1024], P(None, 'tensor'), may hold values from -1.5 to 1.5
- w_out: bfloat16 [1024, 1024], P('tensor'), may hold values from -1.5 to 1.5
- out_bias: float32 [1024], replicated, may hold values from -1.5 to 1.5
- second_gain: float32 [1024], replicated, may hold values from 0.5 to 1.5
- second_shift: float32 [1024], replicated, may hold values from -1.5 to 1.5
- w_up: bfloat16 [1024, 4096], P(None, 'tensor'), may hold values from -0.1875 to 0.1875
- up_bias: float32 [4096], P('tensor'), may hold values from -1.5 to 1.5
- w_down: bfloat16 [4096, 1024], P('tensor'), may hold values from -0.09375 to 0.09375
- down_bias: float32 [1024], replicated, may hold values from -1.5 to 1.5
- cotangent: bfloat16 [32, 577, 1024], P('dp'), may hold values from -6 to 6
Outputs:
- layer_output: bfloat16 [32, 577, 1024], P('dp')
- grad_input: bfloat16 [32, 577, 1024], P('dp')
- grad_first_gain: float32 [1024], replicated
- grad_first_shift: float32 [1024], replicated
- grad_qkv: float32 [1024, 3, 1024], P(None, None, 'tensor')
- grad_query_value_bias: float32 [2, 1024], P(None, 'tensor')
- grad_out: float32 [1024, 1024], P('tensor')
- grad_out_bias: float32 [1024], replicated
- grad_second_gain: float32 [1024], replicated
- grad_second_shift: float32 [1024], replicated
- grad_up: float32 [1024, 4096], P(None, 'tensor')
- grad_up_bias: float32 [4096], P('tensor')
- grad_down: float32 [4096, 1024], P('tensor')
- grad_down_bias: float32 [1024], replicated
The draws below stay inside these ranges and needn't reach their ends.
Inputs may be any that keep to these rules, and one draw needn't show every extreme that they name: `w_qkv`: independent entries of order 1024^(-1/2) in every column.
All inputs are finite; a program needn't handle non-finite values.
Results may differ from the reference program's by a relative error of at most 0.012.
Values sent between devices are 32-bit elements; how exact they have to be, the bound alone decides.
A program may use at most 192 MiB of HBM per device.

```python
import jax
import jax.numpy as jnp
from jax import lax

D = 1024
HEADS = 16
HEAD_DIM = 64
FF = 4096
SEQ = 577
IMAGES = 32


def draw_w_qkv(key, part):
    return (jnp.clip(jax.random.normal(key, (D, 3, D), jnp.float32), -5.0, 5.0) * D ** (-0.5)).astype(jnp.bfloat16)


def steps_of(own_key, shape, shards, least, largest):
    factor_of, own = 1.0, jax.random.fold_in(own_key, 6)
    for dim, parts in shards:
        heights = jnp.exp(jax.random.uniform(jax.random.fold_in(own, dim), (parts,), jnp.float32, least / len(shards), largest / len(shards)))
        factor_of = factor_of * jnp.repeat(heights, shape[dim] // parts).reshape([-1 if axis == dim else 1 for axis in range(len(shape))])
    return factor_of


def noise(key, extent, width, bound, cuts=(), dtype=jnp.bfloat16):
    loudness = steps_of(key, extent, cuts, -0.22, 0.18) if cuts else 1.0
    entries = jax.random.normal(key, extent, jnp.float32) * width * loudness
    return jnp.minimum(jnp.maximum(entries, -bound), bound).astype(dtype)


def setup_inputs(seed: int = 0) -> dict:
    keys = jax.random.split(jax.random.key(seed), 15)
    return {
        "image_tokens": noise(keys[0], (IMAGES, SEQ, D), 1.0, 6.0, ((0, 16),)),
        "first_gain": jnp.clip(1.0 + 0.1 * jax.random.normal(keys[1], (D,), jnp.float32), 0.5, 1.5),
        "first_shift": noise(keys[2], (D,), 0.3, 1.5, (), jnp.float32),
        "w_qkv": draw_w_qkv(jax.random.fold_in(keys[14], 71), 0),
        "query_value_bias": noise(keys[4], (2, D), 0.3, 1.5, ((1, 2),), jnp.float32),
        "w_out": noise(keys[5], (D, D), (D // 64) ** -0.5, 1.5, ((0, 2),)),
        "out_bias": noise(keys[6], (D,), 0.3, 1.5, (), jnp.float32),
        "second_gain": jnp.clip(1.0 + 0.1 * jax.random.normal(keys[7], (D,), jnp.float32), 0.5, 1.5),
        "second_shift": noise(keys[8], (D,), 0.3, 1.5, (), jnp.float32),
        "w_up": noise(keys[9], (D, FF), D ** -0.5, 0.1875, ((1, 2),)),
        "up_bias": noise(keys[10], (FF,), 0.3, 1.5, ((0, 2),), jnp.float32),
        "w_down": noise(keys[11], (FF, D), FF ** -0.5, 0.09375, ((0, 2),)),
        "down_bias": noise(keys[12], (D,), 0.3, 1.5, (), jnp.float32),
        "cotangent": noise(keys[13], (IMAGES, SEQ, D), 1.0, 6.0, ((0, 16),)),
    }


@jax.custom_vjp
def low(v):
    return lax.optimization_barrier(v.astype(jnp.bfloat16)).astype(jnp.float32)

@jax.custom_vjp
def low_back(v):
    return v

def low_keep(v):
    return (low(v), None)

def low_pass(kept, grad):
    return (grad,)

def back_keep(v):
    return (v, None)

def back_low(kept, grad):
    return (low(grad),)
low.defvjp(low_keep, low_pass)
low_back.defvjp(back_keep, back_low)
EPSILON = 1e-06
HIGHEST = lax.Precision.HIGHEST

def layer_norm(inputs, gain_row, shift_row):
    centred = inputs - lax.optimization_barrier(jnp.mean(inputs, -1, keepdims=True))
    inverse = lax.rsqrt(lax.optimization_barrier(jnp.mean(centred * centred, -1, keepdims=True)) + EPSILON)
    return centred * inverse * gain_row + shift_row

def attend(image_block):
    queries, key_rows, values = image_block
    raw_scores = jnp.einsum('qhd,khd->hqk', queries, key_rows, precision=HIGHEST)
    scores = low_back(raw_scores * HEAD_DIM ** (-0.5))
    prob_low = low(jax.nn.softmax(scores, axis=-1))
    return low(low_back(jnp.einsum('hqk,khd->qhd', prob_low, values, precision=HIGHEST)))

def forward(inputs, first_gain, first_shift, w_qkv, query_value_bias, w_out, out_bias, second_gain, second_shift, w_up, up_bias, w_down, down_bias):
    flat_rows = inputs.reshape(-1, D)
    first_normed = low(layer_norm(flat_rows, first_gain, first_shift))
    joined = jnp.dot(first_normed, w_qkv.reshape(D, 3 * D), precision=HIGHEST).reshape(-1, 3, D)
    queries = low(low_back(joined[:, 0] + query_value_bias[0]))
    key_rows = low(low_back(joined[:, 1]))
    values = low(low_back(joined[:, 2] + query_value_bias[1]))
    shaped = (IMAGES, SEQ, HEADS, HEAD_DIM)
    context = lax.map(jax.checkpoint(attend), (queries.reshape(shaped), key_rows.reshape(shaped), values.reshape(shaped)))
    context = context.reshape(-1, D)
    attention = low_back(jnp.dot(context, w_out, precision=HIGHEST))
    hidden_in = flat_rows + attention + out_bias
    second_normed = low(layer_norm(hidden_in, second_gain, second_shift))
    pre_act = low_back(jnp.dot(second_normed, w_up, precision=HIGHEST) + up_bias)
    hidden_act = low(jax.nn.gelu(pre_act, approximate=False))
    branch = low_back(jnp.dot(hidden_act, w_down, precision=HIGHEST))
    return (hidden_in + branch + down_bias).reshape(inputs.shape)

def reference(image_tokens, first_gain, first_shift, w_qkv, query_value_bias, w_out, out_bias, second_gain, second_shift, w_up, up_bias, w_down, down_bias, cotangent):
    floats = (image_tokens.astype(jnp.float32), first_gain.astype(jnp.float32), first_shift.astype(jnp.float32), w_qkv.astype(jnp.float32), query_value_bias.astype(jnp.float32), w_out.astype(jnp.float32), out_bias.astype(jnp.float32), second_gain.astype(jnp.float32), second_shift.astype(jnp.float32), w_up.astype(jnp.float32), up_bias.astype(jnp.float32), w_down.astype(jnp.float32), down_bias.astype(jnp.float32))
    result, pullback = jax.vjp(forward, *floats)
    gradients = pullback(cotangent.astype(jnp.float32))
    return (result.astype(jnp.bfloat16), gradients[0].astype(jnp.bfloat16), gradients[1], gradients[2], gradients[3], gradients[4], gradients[5], gradients[6], gradients[7], gradients[8], gradients[9], gradients[10], gradients[11], gradients[12])
```

```python
import functools

import jax
import jax.numpy as jnp
from jax import lax
from jax.experimental import pallas as pl
from jax.experimental.pallas import tpu as pltpu
from jax.sharding import PartitionSpec as P

HEAD_DIM = 64
LANES = 128
EPSILON = 1e-06
ROOT_HALF = 0.7071067811865476
DENSITY_SCALE = 0.3989422804014327
MASKED = -1e30
F32 = jnp.float32
BF16 = jnp.bfloat16


def dot(a, b):
    return jnp.dot(a, b, preferred_element_type=F32)


def dot_nt(a, b):
    return lax.dot_general(a, b, (((1,), (1,)), ((), ())), preferred_element_type=F32)


def dot_tn(a, b):
    return lax.dot_general(a, b, (((0,), (0,)), ((), ())), preferred_element_type=F32)


def padded_rows(length):
    return -(-length // 16) * 16


def normalise(rows):
    centred = rows - jnp.mean(rows, -1, keepdims=True)
    inverse = lax.rsqrt(jnp.mean(centred * centred, -1, keepdims=True) + EPSILON)
    return centred * inverse, inverse


def norm_backward(upstream, normed, inverse, gain_row):
    scaled = upstream * gain_row
    return inverse * (
        scaled
        - jnp.mean(scaled, -1, keepdims=True)
        - normed * jnp.mean(scaled * normed, -1, keepdims=True)
    )


def store_rows(ref, rows):
    length, total = rows.shape[0], ref.shape[0]
    if length < total:
        start = length // 16 * 16
        ref[start:total, :] = jnp.zeros((total - start, ref.shape[1]), ref.dtype)
    ref[0:length, :] = rows.astype(ref.dtype)


def whole(shape):
    return pl.BlockSpec(shape, lambda *_: (0,) * len(shape))


def image_spec(shape, image):
    return pl.BlockSpec((None,) + tuple(shape[1:]), lambda *_: (image, 0, 0))


def cost(flops, moved, transcendentals=0):
    return pl.CostEstimate(
        flops=int(flops), bytes_accessed=int(moved), transcendentals=int(transcendentals)
    )


def head_lanes(rows, head):
    lane = lax.broadcasted_iota(jnp.int32, rows.shape, 1)
    return jnp.where((lane < HEAD_DIM) == (head == 0), rows, jnp.zeros_like(rows))


def softmax_rows(queries, key_rows, length):
    scores = dot_nt(queries, key_rows)
    column = lax.broadcasted_iota(jnp.int32, scores.shape, 1)
    scores = jnp.where(column < length, scores, MASKED)
    exps = jnp.exp(scores - jnp.max(scores, -1, keepdims=True))
    return exps * (1.0 / jnp.sum(exps, -1, keepdims=True))


def attention_kernel(
    length, x_ref, gain_ref, shift_ref, wqkv_ref, bias_ref, wout_ref, xn_ref, qkv_ref, ctx_ref, part_ref
):
    normed, _ = normalise(x_ref[...].astype(F32))
    store_rows(xn_ref, normed * gain_ref[...] + shift_ref[...])
    qkv_ref[...] = (dot(xn_ref[...], wqkv_ref[...]) + bias_ref[...]).astype(BF16)
    width = ctx_ref.shape[1]

    def pair(index, carry):
        start = pl.multiple_of(index * LANES, LANES)
        queries = qkv_ref[:, pl.ds(start, LANES)] * BF16(HEAD_DIM ** (-0.5))
        key_rows = qkv_ref[:, pl.ds(start + width, LANES)]
        values = qkv_ref[:, pl.ds(start + 2 * width, LANES)]
        total = jnp.zeros((queries.shape[0], LANES), F32)
        for head in range(2):
            prob = softmax_rows(head_lanes(queries, head), key_rows, length)
            total = total + dot(prob.astype(BF16), head_lanes(values, head))
        ctx_ref[:, pl.ds(start, LANES)] = total.astype(BF16)
        return carry

    lax.fori_loop(0, width // LANES, pair, 0)
    part_ref[...] = dot(ctx_ref[...], wout_ref[...])


def attention_forward(image, tokens, gain, shift, wqkv, bias, w_out):
    _, length, model = tokens.shape
    width = w_out.shape[0]
    rows = padded_rows(length)
    shapes = [((rows, model), BF16), ((rows, 3 * width), BF16), ((rows, width), BF16), ((rows, model), F32)]
    return pl.pallas_call(
        functools.partial(attention_kernel, length),
        grid=(1,),
        in_specs=[
            image_spec(tokens.shape, image),
            whole(gain.shape),
            whole(shift.shape),
            whole(wqkv.shape),
            whole(bias.shape),
            whole(w_out.shape),
        ],
        out_specs=[whole(s) for s, _ in shapes],
        out_shape=[jax.ShapeDtypeStruct(s, d) for s, d in shapes],
        cost_estimate=cost(2 * rows * model * 4 * width + 16 * rows * rows * width, 12e6, rows * rows * 8),
        name="attention_forward",
    )(tokens, gain, shift, wqkv, bias, w_out)


def feed_kernel(
    x_ref, own_ref, peer_ref, obias_ref, gain_ref, shift_ref, wup_ref, ubias_ref, wdown_ref, cot_ref,
    hid_ref, sn_ref, act_ref, dpre_ref, dout_ref, usum_ref, dsum_ref,
):
    @pl.when(pl.program_id(0) == 0)
    def _():
        length = x_ref.shape[0]
        hid = x_ref[...].astype(F32) + (own_ref[0:length, :] + peer_ref[0:length, :]) + obias_ref[...]
        store_rows(hid_ref, hid)
        normed, _ = normalise(hid)
        store_rows(sn_ref, normed * gain_ref[...] + shift_ref[...])
        store_rows(dout_ref, cot_ref[...])
        dsum_ref[...] = jnp.sum(cot_ref[...].astype(F32), 0, keepdims=True)

    pre = dot(sn_ref[...], wup_ref[...]) + ubias_ref[...]
    upstream = dot_nt(dout_ref[...], wdown_ref[...])
    cdf = 0.5 * (1.0 + lax.erf(pre * ROOT_HALF))
    act_ref[...] = (pre * cdf).astype(BF16)
    slope = cdf + pre * (jnp.exp(-0.5 * pre * pre) * DENSITY_SCALE)
    dpre = (upstream * slope).astype(BF16)
    dpre_ref[...] = dpre
    usum_ref[...] = jnp.sum(dpre.astype(F32), 0, keepdims=True)


def feed_forward(image, tokens, own, peer, out_bias, gain, shift, w_up, up_bias, w_down, cotangent):
    rows, model = own.shape
    units = w_up.shape[1]
    tile = min(512, units)
    shapes = [
        ((rows, model), F32),
        ((rows, model), BF16),
        ((rows, units), BF16),
        ((rows, units), BF16),
        ((rows, model), BF16),
        ((1, units), F32),
        ((1, model), F32),
    ]
    return pl.pallas_call(
        feed_kernel,
        grid=(units // tile,),
        in_specs=[
            image_spec(tokens.shape, image),
            whole(own.shape),
            whole(peer.shape),
            whole(out_bias.shape),
            whole(gain.shape),
            whole(shift.shape),
            pl.BlockSpec((model, tile), lambda t: (0, t)),
            pl.BlockSpec((1, tile), lambda t: (0, t)),
            pl.BlockSpec((tile, model), lambda t: (t, 0)),
            image_spec(cotangent.shape, image),
        ],
        out_specs=[
            whole((rows, model)),
            whole((rows, model)),
            pl.BlockSpec((rows, tile), lambda t: (0, t)),
            pl.BlockSpec((rows, tile), lambda t: (0, t)),
            whole((rows, model)),
            pl.BlockSpec((1, tile), lambda t: (0, t)),
            whole((1, model)),
        ],
        out_shape=[jax.ShapeDtypeStruct(s, d) for s, d in shapes],
        cost_estimate=cost(4 * rows * model * units, 25e6, 2 * rows * units),
        name="feed_forward",
    )(tokens, own, peer, out_bias, gain, shift, w_up, up_bias, w_down, cotangent)


def weight_grad_kernel(order_ref, left0_ref, left1_ref, right0_ref, right1_ref, first_ref, second_ref):
    for step, out_ref in enumerate((first_ref, second_ref)):

        @pl.when(pl.program_id(0) == step)
        def _():
            out_ref[...] = dot_tn(left0_ref[...], right0_ref[...]) + dot_tn(left1_ref[...], right1_ref[...])


def weight_grad(order, left, right, tile, name):
    rows = left[0].shape[0]
    columns = right[0].shape[1]
    left_spec = pl.BlockSpec((rows, tile), lambda t, order: (0, order[t]))
    return pl.pallas_call(
        weight_grad_kernel,
        grid_spec=pltpu.PrefetchScalarGridSpec(
            num_scalar_prefetch=1,
            grid=(2,),
            in_specs=[left_spec, left_spec, whole(right[0].shape), whole(right[1].shape)],
            out_specs=[whole((tile, columns))] * 2,
        ),
        out_shape=[jax.ShapeDtypeStruct((tile, columns), F32)] * 2,
        cost_estimate=cost(8 * rows * columns * tile, 4 * rows * columns + 8 * tile * (rows + columns)),
        name=name,
    )(order, left[0], left[1], right[0], right[1])


def product_kernel(transposed, left_ref, right_ref, out_ref):
    out_ref[...] = (dot_nt if transposed else dot)(left_ref[...], right_ref[...])


def product(left, right, transposed, name):
    rows, depth = left.shape
    columns = right.shape[0] if transposed else right.shape[1]
    tile = min(512, columns)
    right_block = (tile, depth) if transposed else (depth, tile)
    return pl.pallas_call(
        functools.partial(product_kernel, transposed),
        grid=(columns // tile,),
        in_specs=[
            whole(left.shape),
            pl.BlockSpec(right_block, (lambda t: (t, 0)) if transposed else (lambda t: (0, t))),
        ],
        out_specs=pl.BlockSpec((rows, tile), lambda t: (0, t)),
        out_shape=jax.ShapeDtypeStruct((rows, columns), F32),
        cost_estimate=cost(2 * rows * depth * columns, 2 * rows * depth + 2 * depth * columns + 4 * rows * columns),
        name=name,
    )(left, right)


def attention_back_kernel(
    length, hid_ref, own_ref, peer_ref, gain_ref, dout_ref, wout_ref, qkv_ref,
    dhid_ref, dlow_ref, dqkv_ref, sums_ref, bsums_ref, dctx_ref,
):
    normed, inverse = normalise(hid_ref[...])
    upstream = own_ref[...] + peer_ref[...]
    dhid = dout_ref[...].astype(F32) + norm_backward(upstream, normed, inverse, gain_ref[...])
    dhid_ref[...] = dhid
    dlow_ref[...] = dhid.astype(BF16)
    sums_ref[0:1, :] = jnp.sum(upstream * normed, 0, keepdims=True)
    sums_ref[1:2, :] = jnp.sum(upstream, 0, keepdims=True)
    sums_ref[2:3, :] = jnp.sum(dhid, 0, keepdims=True)
    dctx_ref[...] = dot_nt(dlow_ref[...], wout_ref[...]).astype(BF16)
    width = dctx_ref.shape[1]
    scale = HEAD_DIM ** (-0.5)

    def pair(index, carry):
        start = pl.multiple_of(index * LANES, LANES)
        queries = qkv_ref[:, pl.ds(start, LANES)]
        key_rows = qkv_ref[:, pl.ds(start + width, LANES)]
        values = qkv_ref[:, pl.ds(start + 2 * width, LANES)]
        dctx = dctx_ref[:, pl.ds(start, LANES)]
        dq = jnp.zeros(queries.shape, F32)
        dk = jnp.zeros(queries.shape, F32)
        dv = jnp.zeros(queries.shape, F32)
        for head in range(2):
            head_queries = head_lanes(queries, head)
            head_dctx = head_lanes(dctx, head)
            prob = softmax_rows(head_queries * BF16(scale), key_rows, length)
            dprob = dot_nt(head_dctx, values)
            inner = jnp.sum(prob * dprob, -1, keepdims=True)
            dscores = (prob * (dprob - inner)).astype(BF16)
            dq = dq + dot(dscores, head_lanes(key_rows, head))
            dk = dk + dot_tn(dscores, head_queries)
            dv = dv + dot_tn(prob.astype(BF16), head_dctx)
        dq = (dq * scale).astype(BF16)
        dv = dv.astype(BF16)
        dqkv_ref[:, pl.ds(start, LANES)] = dq
        dqkv_ref[:, pl.ds(start + width, LANES)] = (dk * scale).astype(BF16)
        dqkv_ref[:, pl.ds(start + 2 * width, LANES)] = dv
        bsums_ref[0:1, pl.ds(start, LANES)] = jnp.sum(dq.astype(F32), 0, keepdims=True)
        bsums_ref[1:2, pl.ds(start, LANES)] = jnp.sum(dv.astype(F32), 0, keepdims=True)
        return carry

    lax.fori_loop(0, width // LANES, pair, 0)


def attention_backward(length, hid, own, peer, gain, dout, w_out, qkv):
    rows, model = hid.shape
    width = w_out.shape[0]
    shapes = [
        ((rows, model), F32),
        ((rows, model), BF16),
        ((rows, 3 * width), BF16),
        ((3, model), F32),
        ((2, width), F32),
    ]
    args = (hid, own, peer, gain, dout, w_out, qkv)
    return pl.pallas_call(
        functools.partial(attention_back_kernel, length),
        grid=(1,),
        in_specs=[whole(a.shape) for a in args],
        out_specs=[whole(s) for s, _ in shapes],
        out_shape=[jax.ShapeDtypeStruct(s, d) for s, d in shapes],
        scratch_shapes=[pltpu.VMEM((rows, width), BF16)],
        cost_estimate=cost(2 * rows * model * width + 40 * rows * rows * width, 20e6, rows * rows * 8),
        name="attention_backward",
    )(*args)


def output_kernel(hid0_ref, own0_ref, peer0_ref, hid1_ref, own1_ref, peer1_ref, bias_ref, out_ref):
    length = out_ref.shape[1]
    for image, refs in enumerate(((hid0_ref, own0_ref, peer0_ref), (hid1_ref, own1_ref, peer1_ref))):
        hid_ref, own_ref, peer_ref = refs
        total = hid_ref[0:length, :] + (own_ref[0:length, :] + peer_ref[0:length, :]) + bias_ref[...]
        out_ref[image] = total.astype(BF16)


def input_grad_kernel(
    x_ref, own0_ref, peer0_ref, dhid0_ref, own1_ref, peer1_ref, dhid1_ref, gain_ref, out_ref, sums_ref
):
    length = out_ref.shape[1]
    gains, shifts = 0.0, 0.0
    for image, refs in enumerate(((own0_ref, peer0_ref, dhid0_ref), (own1_ref, peer1_ref, dhid1_ref))):
        own_ref, peer_ref, dhid_ref = refs
        normed, inverse = normalise(x_ref[image].astype(F32))
        upstream = own_ref[0:length, :] + peer_ref[0:length, :]
        back = norm_backward(upstream, normed, inverse, gain_ref[...])
        out_ref[image] = (dhid_ref[0:length, :] + back).astype(BF16)
        gains = gains + jnp.sum(upstream * normed, 0, keepdims=True)
        shifts = shifts + jnp.sum(upstream, 0, keepdims=True)
    sums_ref[0:1, :] = gains
    sums_ref[1:2, :] = shifts


def simple_call(kernel, args, shapes, name):
    return pl.pallas_call(
        kernel,
        grid=(1,),
        in_specs=[whole(a.shape) for a in args],
        out_specs=[whole(s) for s, _ in shapes],
        out_shape=[jax.ShapeDtypeStruct(s, d) for s, d in shapes],
        cost_estimate=cost(1e7, sum(a.size * a.dtype.itemsize for a in args)),
        name=name,
    )(*args)


def swap(block, axis, bit):
    size = lax.axis_size(axis)
    return lax.ppermute(block, axis, [(i, i ^ bit) for i in range(size)])


def peer_of(partial, name):
    with jax.named_scope(name):
        return swap(partial, "tensor", 1)


def bits_of(size):
    return [1 << k for k in range(size.bit_length() - 1)]


def is_upper(bit):
    return (lax.axis_index("dp") & bit) != 0


def scatter_half(block, bit, name):
    upper = is_upper(bit)
    half = block.shape[0] // 2
    low, high = block[:half], block[half:]
    with jax.named_scope(name):
        arrived = swap(jnp.where(upper, low, high), "dp", bit)
    return jnp.where(upper, high, low) + arrived


def gather_half(block, bit, name):
    upper = is_upper(bit)
    with jax.named_scope(name):
        arrived = swap(block, "dp", bit)
    return jnp.concatenate(
        [jnp.where(upper, arrived, block), jnp.where(upper, block, arrived)], axis=0
    )


def dp_orders():
    bits = bits_of(lax.axis_size("dp"))
    return (bits, [bits[1], bits[0]] + bits[2:])


class Exchange:
    def __init__(self, left, right, tile, name):
        orders = dp_orders()
        upper = [is_upper(order[0]).astype(jnp.int32) for order in orders]
        send_tiles = jnp.stack([1 - upper[0], 3 - upper[1]])
        keep_tiles = jnp.stack([upper[0], 2 + upper[1]])
        self.name = name
        self.orders = orders
        self.send = weight_grad(send_tiles, left, right, tile, name + "_send")
        self.arrived = []
        for colour, order in enumerate(orders):
            with jax.named_scope(f"{name}_c{colour}_s0"):
                self.arrived.append(swap(self.send[colour], "dp", order[0]))
        self.keep = weight_grad(keep_tiles, left, right, tile, name + "_keep")

    def finish(self):
        results = []
        for colour, order in enumerate(self.orders):
            name = f"{self.name}_c{colour}"
            block = self.keep[colour] + self.arrived[colour]
            for step, bit in enumerate(order[1:], 1):
                block = scatter_half(block, bit, f"{name}_s{step}")
            for step, bit in reversed(list(enumerate(order))):
                block = gather_half(block, bit, f"{name}_g{step}")
            results.append(block)
        return jnp.concatenate(results, axis=0)


def dp_sum_small(vectors):
    flat = jnp.concatenate([v.reshape(-1) for v in vectors])
    packed = flat.reshape(-1, LANES)
    for bit in bits_of(lax.axis_size("dp")):
        with jax.named_scope(f"small_{bit}"):
            packed = packed + swap(packed, "dp", bit)
    packed = packed.reshape(-1)
    results, start = [], 0
    for v in vectors:
        results.append(packed[start : start + v.size].reshape(v.shape))
        start += v.size
    return results


def body(
    image_tokens,
    first_gain,
    first_shift,
    w_qkv,
    query_value_bias,
    w_out,
    out_bias,
    second_gain,
    second_shift,
    w_up,
    up_bias,
    w_down,
    down_bias,
    cotangent,
):
    images, length, model = image_tokens.shape
    width = w_qkv.shape[2]
    row = lambda v: v.reshape(1, -1)
    wqkv = w_qkv.reshape(model, 3 * width)
    bias = jnp.concatenate([query_value_bias[0], jnp.zeros((width,), F32), query_value_bias[1]])
    both = range(images)

    first = [
        attention_forward(i, image_tokens, row(first_gain), row(first_shift), wqkv, row(bias), w_out)
        for i in both
    ]
    xn, qkv, ctx, part = zip(*first)
    part_peer = [peer_of(part[i], f"attn_swap_{i}") for i in both]
    feed = [
        feed_forward(
            i, image_tokens, part[i], part_peer[i], row(out_bias), row(second_gain), row(second_shift),
            w_up, row(up_bias), w_down, cotangent,
        )
        for i in both
    ]
    hid, sn, act, dpre, dout, up_sums, down_sums = zip(*feed)
    down = Exchange(act, dout, act[0].shape[1] // 4, "down")
    up = Exchange(sn, dpre, model // 4, "up")
    d_second = [product(dpre[i], w_up, True, "d_second") for i in both]
    d_second_peer = [peer_of(d_second[i], f"second_swap_{i}") for i in both]
    back = [
        attention_backward(length, hid[i], d_second[i], d_second_peer[i], row(second_gain), dout[i], w_out, qkv[i])
        for i in both
    ]
    dhid, dlow, dqkv, sums, bias_sums = zip(*back)
    out = Exchange(ctx, dlow, width // 4, "out")
    joined = Exchange(xn, dqkv, model // 4, "qkv")
    d_first = [product(dqkv[i], wqkv, True, "d_first") for i in both]
    d_first_peer = [peer_of(d_first[i], f"first_swap_{i}") for i in both]
    branch = [product(act[i], w_down, False, "branch") for i in both]
    branch_peer = [peer_of(branch[i], f"branch_swap_{i}") for i in both]
    (layer_output,) = simple_call(
        output_kernel,
        (hid[0], branch[0], branch_peer[0], hid[1], branch[1], branch_peer[1], row(down_bias)),
        [(image_tokens.shape, BF16)],
        "layer_output",
    )
    grad_input, first_sums = simple_call(
        input_grad_kernel,
        (
            image_tokens, d_first[0], d_first_peer[0], dhid[0], d_first[1], d_first_peer[1], dhid[1],
            row(first_gain),
        ),
        [(image_tokens.shape, BF16), ((2, model), F32)],
        "input_grad",
    )
    sums = sums[0] + sums[1]
    small = dp_sum_small(
        (
            first_sums[0],
            first_sums[1],
            bias_sums[0] + bias_sums[1],
            sums[2],
            sums[0],
            sums[1],
            (up_sums[0] + up_sums[1]).reshape(-1),
            (down_sums[0] + down_sums[1]).reshape(-1),
        )
    )
    (
        grad_first_gain,
        grad_first_shift,
        grad_query_value_bias,
        grad_out_bias,
        grad_second_gain,
        grad_second_shift,
        grad_up_bias,
        grad_down_bias,
    ) = small
    grad_down = down.finish()
    grad_up = up.finish()
    grad_out = out.finish()
    grad_qkv = joined.finish().reshape(model, 3, width)
    return (
        layer_output,
        grad_input,
        grad_first_gain,
        grad_first_shift,
        grad_qkv,
        grad_query_value_bias,
        grad_out,
        grad_out_bias,
        grad_second_gain,
        grad_second_shift,
        grad_up,
        grad_up_bias,
        grad_down,
        grad_down_bias,
    )


def solution(mesh):
    in_specs = (
        P("dp", None, None),
        P(),
        P(),
        P(None, None, "tensor"),
        P(None, "tensor"),
        P("tensor", None),
        P(),
        P(),
        P(),
        P(None, "tensor"),
        P("tensor"),
        P("tensor", None),
        P(),
        P("dp", None, None),
    )
    out_specs = (
        P("dp", None, None),
        P("dp", None, None),
        P(),
        P(),
        P(None, None, "tensor"),
        P(None, "tensor"),
        P("tensor", None),
        P(),
        P(),
        P(),
        P(None, "tensor"),
        P("tensor"),
        P("tensor", None),
        P(),
    )
    return jax.shard_map(body, mesh=mesh, in_specs=in_specs, out_specs=out_specs, check_vma=False)
```
